32 devices in a mesh: gx: 8 (over z, x), gy: 4 (over y, core).
Axes of the slice: x: 2, y: 2, z: 4, core: 2. Of those that a mesh axis runs over, the one named last changes fastest.
Arguments:
- dense_grads: float32 [32, 256, 1024], P(('gx', 'gy')), may hold values from -6 to 6
- dense_param: float32 [256, 1024], P(('gx', 'gy')), may hold values from -6 to 6
- dense_acc: float32 [256, 1024], P(('gx', 'gy'))
- table: float32 [131072, 128], P(('gx', 'gy')), may hold values from -6 to 6
- row_acc: float32 [131072], P(('gx', 'gy'))
- touched: int32 [16384], P(('gx', 'gy')), may hold values from 0 to 4095, as said below
- emb_grads: float32 [16384, 128], P(('gx', 'gy'))
Outputs:
- new_dense: float32 [256, 1024], P(('gx', 'gy'))
- new_dense_acc: float32 [256, 1024], P(('gx', 'gy'))
- new_table: float32 [131072, 128], P(('gx', 'gy'))
- new_row_acc: float32 [131072], P(('gx', 'gy'))
The draws below stay inside these ranges and needn't reach their ends.
Inputs may be any that keep to these rules, and one draw needn't show every extreme that they name: `touched`: within one device's 512 entries no row number repeats.
All inputs are finite; a program needn't handle non-finite values.
Results may differ from the reference program's by a relative error of at most 0.000022.
Values sent between devices are 32-bit elements; how exact they have to be, the bound alone decides.
No kernel may reach another device: no remote copies, remote signals or barrier semaphores. Data moves between devices by JAX's collectives and lax.ppermute only.
A program may use at most 128 MiB of HBM per device.

```python
import jax
import jax.numpy as jnp
from jax import lax

H = 1024
EMB_DIM = 128
ROWS_DEV = 4096
TOUCH_DEV = 512
SHARDS = 32
DENSE_ROWS = 256
TABLE_ROWS = 131072
TOUCHED = 16384


def draw_touched(key, part):
    keys = jax.random.split(jax.random.fold_in(key, 11), SHARDS)
    picks = jax.vmap(lambda single: jax.random.permutation(single, ROWS_DEV)[:TOUCH_DEV])(keys)
    return picks.reshape(TOUCHED).astype(jnp.int32)


def draw_emb_grads(key, part):
    first = jax.random.fold_in(jax.random.fold_in(key, 23), 0)
    owner = jnp.arange(TOUCHED, dtype=jnp.float32) // TOUCH_DEV
    ramp = 1.0 + 2.0 * owner / max(SHARDS - 1, 1)
    values = jax.random.normal(first, (TOUCHED, EMB_DIM), jnp.float32)
    scale = ramp / (8.0 * jnp.sqrt(jnp.float32(SHARDS)))
    return (values * scale[:, None]).astype(jnp.float32)


def draw_dense_acc(key, part):
    logs = jax.random.uniform(jax.random.fold_in(key, 37), (DENSE_ROWS, H), jnp.float32, jnp.log(0.0005), jnp.log(0.05))
    return (jnp.exp(logs) / jnp.float32(SHARDS)).astype(jnp.float32)


def draw_row_acc(key, part):
    logs = jax.random.uniform(jax.random.fold_in(key, 41), (TABLE_ROWS,), jnp.float32, jnp.log(1e-05), jnp.log(0.001))
    return (jnp.exp(logs) / jnp.float32(SHARDS)).astype(jnp.float32)


def spiked(drawn, rng, source, target, shards_of, factor):
    owner, partner = [(jnp.arange(drawn.shape[dim]) // (drawn.shape[dim] // shards_of)).reshape([-1 if axis == dim else 1 for axis in range(drawn.ndim)]) for dim in (source, target)]
    chosen = jax.random.permutation(rng, shards_of)[partner]
    strong = (owner == chosen) | (owner == (partner + shards_of // 2) % shards_of)
    return jnp.where(strong, factor * drawn, drawn)


def steps_of(key, dims, cuts, smallest, top_value):
    loudness, own = 1.0, jax.random.fold_in(key, 6)
    for position, shards_of in cuts:
        heights = jnp.exp(jax.random.uniform(jax.random.fold_in(own, position), (shards_of,), jnp.float32, smallest / len(cuts), top_value / len(cuts)))
        loudness = loudness * jnp.repeat(heights, dims[position] // shards_of).reshape([-1 if axis == position else 1 for axis in range(len(dims))])
    return loudness


def centred(stream_key, shape, scale, most, pieces=(), kind=jnp.bfloat16):
    drawn = scale * jax.random.normal(stream_key, shape, jnp.float32)
    if pieces:
        drawn = drawn * steps_of(stream_key, shape, pieces, -0.22, 0.18)
    return jnp.clip(drawn, -most, most).astype(kind)


def noise_with(rng, dims, scale, most, cuts, heavy, kind=jnp.bfloat16):
    result = scale * jax.random.normal(rng, dims, jnp.float32)
    if cuts:
        result = result * steps_of(rng, dims, cuts, -0.22, 0.18)
    return jnp.clip(spiked(result, jax.random.fold_in(rng, 3), *heavy), -most, most).astype(kind)


def setup_inputs(seed: int = 0) -> dict:
    key_list = jax.random.split(jax.random.key(seed), 8)
    return {
        "dense_grads": noise_with(key_list[0], (SHARDS, DENSE_ROWS, H), 1.0, 6.0, ((0, 32),), (0, 1, 32, 2.75), jnp.float32),
        "dense_param": centred(key_list[1], (DENSE_ROWS, H), 1.0, 6.0, ((0, 32),), jnp.float32),
        "dense_acc": draw_dense_acc(jax.random.fold_in(key_list[7], 71), 0),
        "table": centred(key_list[3], (TABLE_ROWS, EMB_DIM), 1.0, 6.0, ((0, 32),), jnp.float32),
        "row_acc": draw_row_acc(jax.random.fold_in(key_list[7], 71), 0),
        "touched": draw_touched(jax.random.fold_in(key_list[7], 71), 0),
        "emb_grads": draw_emb_grads(jax.random.fold_in(key_list[7], 71), 0),
    }


learn_rate = 0.5
max_norm = 8.0
epsilon = 1e-10

def reference(dense_grads, dense_param, dense_acc, table, row_acc, touched, emb_grads):
    mean_grad = lax.optimization_barrier(jnp.sum(dense_grads, axis=0)) / jnp.float32(SHARDS)
    norm_sq = jnp.sum(mean_grad * mean_grad) + jnp.sum(emb_grads * emb_grads)
    clip = jnp.minimum(jnp.float32(1.0), max_norm / (jnp.sqrt(norm_sq) + 1e-06))
    scaled = clip * mean_grad
    new_dense_acc = dense_acc + scaled * scaled
    new_dense = dense_param - learn_rate * scaled / (jnp.sqrt(new_dense_acc) + epsilon)
    owner = (jnp.arange(TOUCHED, dtype=jnp.int32) // TOUCH_DEV).astype(jnp.int32)
    global_rows = (owner * ROWS_DEV + touched).astype(jnp.int32)
    row_grads = clip * emb_grads
    square_mean = lax.optimization_barrier(jnp.mean(row_grads * row_grads, axis=1))
    updated_acc = row_acc[global_rows] + square_mean
    new_row_acc = row_acc.at[global_rows].set(updated_acc)
    updated_rows = table[global_rows] - learn_rate * row_grads / (jnp.sqrt(updated_acc) + epsilon)[:, None]
    new_table = table.at[global_rows].set(updated_rows)
    return (new_dense, new_dense_acc, new_table, new_row_acc)
```

```python
import jax
import jax.numpy as jnp
from jax import lax
from jax.sharding import PartitionSpec as P

learn_rate = 0.5
max_norm = 8.0
epsilon = 1e-10
axes = ("gx", "gy")
lanes = 128


def swap(value, mask):
    count = lax.axis_size(axes)
    return lax.ppermute(value, axes, [(i, i ^ mask) for i in range(count)])


def pick(value, live, bits, flip):
    index = lax.axis_index(axes)
    for bit in bits:
        chosen = (index >> bit) & 1
        if (flip >> bit) & 1:
            chosen = 1 - chosen
        value = lax.dynamic_index_in_dim(value, chosen, live.index(bit), keepdims=False)
        live = [other for other in live if other != bit]
    return value


def reduced(local_grad, embed_square):
    count = lax.axis_size(axes)
    total_bits = count.bit_length() - 1
    own_rows = local_grad.shape[0] // count
    width = local_grad.shape[1]
    data = local_grad.reshape((2,) * total_bits + (own_rows, width))
    live = list(range(total_bits))[::-1]
    last = list(range(max(total_bits - 2, 3), total_bits))
    rounds = [[0], [1, 2]] + [[bit] for bit in range(3, last[0])]
    for bits in rounds:
        masks = [sum(((code >> j) & 1) << bit for j, bit in enumerate(bits)) for code in range(1, 2 ** len(bits))]
        arrived = [swap(pick(data, live, bits, mask), mask) for mask in masks[::-1]]
        data = pick(data, live, bits, 0)
        for part in arrived:
            data = data + part
        live = [bit for bit in live if bit not in bits]
    lead = data.shape[:-2]
    tile = jnp.zeros(lead + (own_rows, lanes), jnp.float32)
    tile = tile.at[(0,) * len(lead)].set(embed_square)
    data = jnp.concatenate([data, tile], axis=-1)
    for bit in last:
        data = data + swap(data, 1 << bit)
    mean = data[..., :width] / jnp.float32(count)
    squares = jnp.sum(jnp.square(mean).reshape((-1, own_rows, width // lanes, lanes)), axis=(0, 2))
    partial = squares + data[..., width:][(0,) * len(lead)]
    for bit in [bit for bits in rounds[::-1] for bit in bits]:
        partial = partial + swap(partial, 1 << bit)
    return pick(mean, live, live, 0), partial


def body(dense_grads, dense_param, dense_acc, table, row_acc, touched, emb_grads):
    own_rows = dense_param.shape[0]
    square = emb_grads * emb_grads
    embed_square = jnp.sum(square.reshape((-1, own_rows, emb_grads.shape[1])), axis=0)
    row_square = jnp.mean(square, axis=1)
    square_table = jnp.zeros_like(row_acc).at[touched].set(row_square, unique_indices=True)
    old_acc = row_acc[touched]
    old_rows = table[touched]

    mean_grad, partial = reduced(dense_grads[0], embed_square)
    norm_sq = jnp.sum(partial)
    clip = jnp.minimum(jnp.float32(1.0), max_norm / (jnp.sqrt(norm_sq) + 1e-06))
    scaled = clip * mean_grad
    new_dense_acc = dense_acc + scaled * scaled
    new_dense = dense_param - learn_rate * scaled / (jnp.sqrt(new_dense_acc) + epsilon)
    clip_sq = clip * clip
    new_row_acc = row_acc + jnp.where(clip > 0, clip_sq * square_table, 0.0)
    updated_acc = old_acc + jnp.where(clip > 0, clip_sq * row_square, 0.0)
    updated_rows = old_rows - learn_rate * (clip * emb_grads) / (jnp.sqrt(updated_acc) + epsilon)[:, None]
    new_table = table.at[touched].set(updated_rows, unique_indices=True)
    return (new_dense, new_dense_acc, new_table, new_row_acc)


def solution(mesh):
    return jax.shard_map(
        body,
        mesh=mesh,
        in_specs=(
            P(axes, None, None),
            P(axes, None),
            P(axes, None),
            P(axes, None),
            P(axes),
            P(axes),
            P(axes, None),
        ),
        out_specs=(P(axes, None), P(axes, None), P(axes, None), P(axes)),
        check_vma=False,
    )
```

```python
import jax
import jax.numpy as jnp
from jax import lax
from jax.experimental import pallas as pl
from jax.experimental.pallas import tpu as pltpu
from jax.sharding import PartitionSpec as P

learn_rate = 0.5
max_norm = 8.0
epsilon = 1e-10
axes = ("gx", "gy")
lanes = 128


def swap(value, mask):
    count = lax.axis_size(axes)
    return lax.ppermute(value, axes, [(i, i ^ mask) for i in range(count)])


def pick(value, live, bits, flip):
    index = lax.axis_index(axes)
    for bit in bits:
        chosen = (index >> bit) & 1
        if (flip >> bit) & 1:
            chosen = 1 - chosen
        value = lax.dynamic_index_in_dim(value, chosen, live.index(bit), keepdims=False)
        live = [other for other in live if other != bit]
    return value


def masks_of(bits):
    return [sum(((code >> j) & 1) << bit for j, bit in enumerate(bits)) for code in range(1, 2 ** len(bits))]


def reduced(local_grad, touched, square, gather):
    count = lax.axis_size(axes)
    total_bits = count.bit_length() - 1
    own_rows = local_grad.shape[0] // count
    width = local_grad.shape[1]
    data = local_grad.reshape((2,) * total_bits + (own_rows, width))
    live = list(range(total_bits))[::-1]
    last = list(range(max(total_bits - 2, 3), total_bits))
    rounds = [[0], [1, 2]] + [[bit] for bit in range(3, last[0])]
    for bits in rounds:
        if len(bits) > 1:
            data, touched = lax.optimization_barrier((data, touched))
            row_square, square_table, embed_square = square(touched)
        arrived = [swap(pick(data, live, bits, mask), mask) for mask in masks_of(bits)[::-1]]
        data = pick(data, live, bits, 0)
        for part in arrived:
            data = data + part
        live = [bit for bit in live if bit not in bits]
    lead = data.shape[:-2]
    tile = jnp.zeros(lead + (own_rows, lanes), jnp.float32)
    tile = tile.at[(0,) * len(lead)].set(embed_square)
    data = jnp.concatenate([data, tile], axis=-1)
    for bit in last[:-1]:
        data = data + swap(data, 1 << bit)
    data, touched = lax.optimization_barrier((data, touched))
    gathered = gather(touched)
    data = data + swap(data, 1 << last[-1])
    copy, old_rows, old_acc = gathered
    data, old_rows = lax.optimization_barrier((data, old_rows))
    mean = data[..., :width] / jnp.float32(count)
    squares = jnp.sum(jnp.square(mean).reshape((-1, own_rows, width // lanes, lanes)), axis=(0, 2))
    partial = squares + data[..., width:][(0,) * len(lead)]
    for bits in rounds[::-1]:
        arrived = [swap(partial, mask) for mask in masks_of(bits)[::-1]]
        for part in arrived:
            partial = partial + part
    return pick(mean, live, live, 0), partial, (copy, old_rows, old_acc, row_square, square_table)


unroll = 8
pieces = 8


def square_kernel(touched, grads, row_square, square_table, embed_square):
    square = jnp.square(grads[...])
    embed_square[...] = jnp.sum(square.reshape((-1,) + embed_square.shape), axis=0)
    square_table[...] = jnp.zeros_like(square_table)
    total = jnp.sum(square, axis=1, keepdims=True)
    row_square[...] = jnp.broadcast_to(total / grads.shape[1], row_square.shape)
    lane = lax.broadcasted_iota(jnp.int32, (1, lanes), 1)

    def spread(step, _):
        base = pl.multiple_of(step * unroll, unroll)
        places = [touched[base + j] for j in range(unroll)]
        here = [lane == (place & (lanes - 1)) for place in places]
        values = [row_square[pl.ds(base + j, 1), :] for j in range(unroll)]
        for j in range(unroll):
            row = pl.ds(places[j] // lanes, 1)
            square_table[row, :] = jnp.where(here[j], values[j], square_table[row, :])
        return 0

    lax.fori_loop(0, grads.shape[0] // unroll, spread, 0)


def square_rows(touched, grads, table_rows):
    vmem = pl.BlockSpec(memory_space=pltpu.VMEM)
    return pl.pallas_call(
        square_kernel,
        out_shape=(
            pltpu.VMEM(grads.shape, jnp.float32),
            pltpu.VMEM((table_rows // lanes, lanes), jnp.float32),
            pltpu.VMEM((8, lanes), jnp.float32),
        ),
        in_specs=[pl.BlockSpec(memory_space=pltpu.SMEM), vmem],
        out_specs=(vmem,) * 3,
        name="square",
    )(touched, grads)


def gather_kernel(touched, table, row_acc, copy, old_rows, old_acc, held, loaded, stored):
    height = held.shape[0] // pieces
    parts = [pl.ds(k * height, height) for k in range(pieces)]
    loads = [pltpu.make_async_copy(table.at[part], held.at[part], loaded.at[k]) for k, part in enumerate(parts)]
    stores = [pltpu.make_async_copy(held.at[part], copy.at[part], stored.at[k]) for k, part in enumerate(parts)]
    for load in loads:
        load.start()
    lane = lax.broadcasted_iota(jnp.int32, (1, lanes), 1)

    def collect(step, _):
        base = pl.multiple_of(step * unroll, unroll)
        places = [touched[base + j] for j in range(unroll)]
        found = [row_acc[pl.ds(place // lanes, 1), :] for place in places]
        for j in range(unroll):
            old_acc[pl.ds(base + j, 1), :] = jnp.where(lane == (places[j] & (lanes - 1)), found[j], 0.0)
        return 0

    lax.fori_loop(0, old_acc.shape[0] // unroll, collect, 0)
    for load, store in zip(loads, stores):
        load.wait()
        store.start()
    chosen = jnp.sum(old_acc[...], axis=1, keepdims=True)
    old_acc[...] = jnp.broadcast_to(chosen, old_acc.shape)

    def gather(step, _):
        base = pl.multiple_of(step * unroll, unroll)
        rows = [held[pl.ds(touched[base + j], 1), :] for j in range(unroll)]
        for j in range(unroll):
            old_rows[pl.ds(base + j, 1), :] = rows[j]
        return 0

    lax.fori_loop(0, old_rows.shape[0] // unroll, gather, 0)
    for store in stores:
        store.wait()


def gather_rows(touched, table, row_acc):
    vmem = pl.BlockSpec(memory_space=pltpu.VMEM)
    any_space = pl.BlockSpec(memory_space=pl.ANY)
    return pl.pallas_call(
        gather_kernel,
        out_shape=(
            jax.ShapeDtypeStruct(table.shape, jnp.float32),
            pltpu.VMEM(touched.shape + table.shape[1:], jnp.float32),
            pltpu.VMEM(touched.shape + table.shape[1:], jnp.float32),
        ),
        in_specs=[pl.BlockSpec(memory_space=pltpu.SMEM), any_space, vmem],
        out_specs=(any_space, vmem, vmem),
        scratch_shapes=[
            pltpu.VMEM(table.shape, jnp.float32),
            pltpu.SemaphoreType.DMA((pieces,)),
            pltpu.SemaphoreType.DMA((pieces,)),
        ],
        name="gather",
    )(touched, table, pltpu.with_memory_space_constraint(row_acc, pltpu.VMEM))


def update_kernel(
    touched, partial, mean, param, acc, grads, old_rows, old_acc, row_square, square_table, row_acc, copy,
    new_param, new_acc, new_row_acc, new_table, rows, copied,
):
    norm_sq = jnp.sum(partial[...], keepdims=True)
    clip = jnp.minimum(jnp.float32(1.0), max_norm / (jnp.sqrt(norm_sq) + 1e-06))
    clip_sq = clip * clip
    updated = old_acc[...] + jnp.where(clip > 0, clip_sq * row_square[...], 0.0)
    rows[...] = old_rows[...] - learn_rate * (clip * grads[...]) / (jnp.sqrt(updated) + epsilon)

    def scatter(step, _):
        base = pl.multiple_of(step * unroll, unroll)
        for j in range(unroll):
            place = touched[base + j]
            pltpu.make_async_copy(rows.at[pl.ds(base + j, 1)], new_table.at[pl.ds(place, 1)], copied).start()
        return 0

    lax.fori_loop(0, grads.shape[0] // unroll, scatter, 0)
    scaled = clip * mean[...]
    grown = acc[...] + scaled * scaled
    new_acc[...] = grown
    new_param[...] = param[...] - learn_rate * scaled / (jnp.sqrt(grown) + epsilon)
    new_row_acc[...] = row_acc[...] + jnp.where(clip > 0, clip_sq * square_table[...], 0.0)
    pltpu.make_async_copy(rows, new_table.at[pl.ds(0, rows.shape[0])], copied).wait()


def update(touched, partial, mean, param, acc, grads, prepared, row_acc):
    copy = prepared[0]
    old_rows, old_acc, row_square, square_table = [
        pltpu.with_memory_space_constraint(value, pltpu.VMEM) for value in prepared[1:]
    ]
    vmem = pl.BlockSpec(memory_space=pltpu.VMEM)
    any_space = pl.BlockSpec(memory_space=pl.ANY)
    return pl.pallas_call(
        update_kernel,
        out_shape=(
            jax.ShapeDtypeStruct(param.shape, jnp.float32),
            jax.ShapeDtypeStruct(acc.shape, jnp.float32),
            jax.ShapeDtypeStruct(row_acc.shape, jnp.float32),
            jax.ShapeDtypeStruct(copy.shape, jnp.float32),
        ),
        in_specs=[pl.BlockSpec(memory_space=pltpu.SMEM)] + [vmem] * 10 + [any_space],
        out_specs=(vmem, vmem, vmem, any_space),
        input_output_aliases={11: 3},
        scratch_shapes=[pltpu.VMEM(grads.shape, jnp.float32), pltpu.SemaphoreType.DMA],
        name="update",
    )(touched, partial, mean, param, acc, grads, old_rows, old_acc, row_square, square_table, row_acc, copy)


def body(dense_grads, dense_param, dense_acc, table, row_acc, touched, emb_grads):
    flat_acc = row_acc.reshape((-1, lanes))
    mean_grad, partial, prepared = reduced(
        dense_grads[0],
        touched,
        lambda places: square_rows(places, emb_grads, row_acc.shape[0]),
        lambda places: gather_rows(places, table, flat_acc),
    )
    close = [
        pltpu.with_memory_space_constraint(value, pltpu.VMEM)
        for value in (partial, mean_grad, dense_param, dense_acc, emb_grads)
    ]
    new_dense, new_dense_acc, new_row_acc, new_table = update(
        touched, *close, prepared, pltpu.with_memory_space_constraint(flat_acc, pltpu.VMEM)
    )
    return (new_dense, new_dense_acc, new_table, new_row_acc.reshape(row_acc.shape))


def solution(mesh):
    return jax.shard_map(
        body,
        mesh=mesh,
        in_specs=(
            P(axes, None, None),
            P(axes, None),
            P(axes, None),
            P(axes, None),
            P(axes),
            P(axes),
            P(axes, None),
        ),
        out_specs=(P(axes, None), P(axes, None), P(axes, None), P(axes)),
        check_vma=False,
    )
```
